256 devices in a mesh: clip: 32 (over z_lo, x, core), tm: 8 (over y, z_hi).
Axes of the slice: x: 4, y: 4, z: 8 (z_hi: 2, z_lo: 4; z = z_hi * 4 + z_lo), core: 2. Of those that a mesh axis runs over, the one named last changes fastest.
Arguments:
- block_input: bfloat16 [32, 16, 32, 4096], P('clip', 'tm'), may hold values from -6 to 6
- input_cache: bfloat16 [32, 2, 32, 4096], P('clip'), may hold values from -6 to 6
- middle_cache: bfloat16 [32, 2, 32, 4096], P('clip'), may hold values from -6 to 6
- first_weight: bfloat16 [3, 3, 3, 64, 64], replicated, may hold values from -0.15625 to 0.15625
- first_bias: float32 [64], replicated, may hold values from -3 to 3
- second_weight: bfloat16 [3, 3, 3, 64, 64], replicated, may hold values from -0.15625 to 0.15625
- cotangent: bfloat16 [32, 16, 32, 4096], P('clip', 'tm'), may hold values from -6 to 6
Outputs:
- input_grad: bfloat16 [32, 16, 32, 4096], P('clip', 'tm')
- input_cache_grad: bfloat16 [32, 2, 32, 4096], P('clip', None, 'tm')
- middle_cache_grad: bfloat16 [32, 2, 32, 4096], P('clip', None, 'tm')
- first_weight_grad: float32 [3, 3, 3, 64, 64], replicated
- second_weight_grad: float32 [3, 3, 3, 64, 64], replicated
The draws below stay inside these ranges and needn't reach their ends.
All inputs are finite; a program needn't handle non-finite values.
Results may differ from the reference program's by a relative error of at most 0.009.
Values may be sent and summed in bfloat16 or wider, within the bound.
A program may use at most 128 MiB of HBM per device.

```python
import jax
import jax.numpy as jnp
from jax import lax

C = 64
H = 32
W = 64
CLIPS = 32
FRAMES = 16


def steps_of(key, extent, pieces, smallest, high):
    factor_of, own = 1.0, jax.random.fold_in(key, 6)
    for position, blocks in pieces:
        heights = jnp.exp(jax.random.uniform(jax.random.fold_in(own, position), (blocks,), jnp.float32, smallest / len(pieces), high / len(pieces)))
        factor_of = factor_of * jnp.repeat(heights, extent[position] // blocks).reshape([-1 if axis == position else 1 for axis in range(len(extent))])
    return factor_of


def normal_values(key, shape, scale, limit, shards=(), kind=jnp.bfloat16):
    result = jax.random.normal(key, shape, jnp.float32) * scale
    if len(shards) > 0:
        result = steps_of(key, shape, shards, -0.22, 0.18) * result
    return jnp.clip(result, min=-limit, max=limit).astype(kind)


def setup_inputs(seed: int = 0) -> dict:
    key_of = jax.random.split(jax.random.key(seed), 8)
    return {
        "block_input": normal_values(key_of[0], (CLIPS, FRAMES, H, W * C), 1.0, 6.0, ((0, 32), (1, 8))),
        "input_cache": normal_values(key_of[1], (CLIPS, 2, H, W * C), 1.0, 6.0, ((0, 32),)),
        "middle_cache": normal_values(key_of[2], (CLIPS, 2, H, W * C), 1.0, 6.0, ((0, 32),)),
        "first_weight": normal_values(key_of[3], (3, 3, 3, C, C), (27 * C) ** -0.5, 0.15625),
        "first_bias": normal_values(key_of[4], (C,), 0.5, 3.0, (), jnp.float32),
        "second_weight": normal_values(key_of[5], (3, 3, 3, C, C), (27 * C) ** -0.5, 0.15625),
        "cotangent": normal_values(key_of[6], (CLIPS, FRAMES, H, W * C), 1.0, 6.0, ((0, 32), (1, 8))),
    }


def conv(source, weight):
    return lax.conv_general_dilated(source.astype(jnp.float32), weight.astype(jnp.float32), (1, 1, 1), ((0, 0), (1, 1), (1, 1)), dimension_numbers=('NDHWC', 'DHWIO', 'NDHWC'), precision=lax.Precision.HIGHEST)

def silu_slope(value):
    logistic = jax.nn.sigmoid(value)
    return logistic * (1.0 + value * (1.0 - logistic))

def reference(block_input, input_cache, middle_cache, first_weight, first_bias, second_weight, cotangent):

    def one_clip(items):
        block, cache_first, cache_second, upstream = items
        shaped = block.reshape(1, FRAMES, H, W, C)
        extended = jnp.concatenate([cache_first.reshape(1, 2, H, W, C), shaped], axis=1)
        activated = jax.nn.silu(extended.astype(jnp.float32)).astype(jnp.bfloat16)
        pre = conv(activated, first_weight) + first_bias
        middle = jax.nn.silu(pre).astype(jnp.bfloat16)
        middle_ext = jnp.concatenate([cache_second.reshape(1, 2, H, W, C), middle], axis=1)
        upstream_f = upstream.reshape(1, FRAMES, H, W, C).astype(jnp.float32)
        unused_out, pull_second = jax.vjp(conv, middle_ext.astype(jnp.float32), second_weight.astype(jnp.float32))
        middle_ext_grad, second_sum = pull_second(upstream_f)
        pre_grad = (middle_ext_grad[:, 2:] * silu_slope(pre)).astype(jnp.bfloat16)
        unused_pre, pull_first = jax.vjp(conv, activated.astype(jnp.float32), first_weight.astype(jnp.float32))
        activated_grad, first_sum = pull_first(pre_grad.astype(jnp.float32))
        extended_grad = activated_grad * silu_slope(extended.astype(jnp.float32))
        input_grad = (upstream_f + extended_grad[:, 2:]).astype(jnp.bfloat16).reshape(FRAMES, H, W * C)
        input_cache_grad = extended_grad[:, :2].astype(jnp.bfloat16).reshape(2, H, W * C)
        middle_cache_grad = middle_ext_grad[:, :2].astype(jnp.bfloat16).reshape(2, H, W * C)
        return (input_grad, input_cache_grad, middle_cache_grad, first_sum, second_sum)
    grads, cache_a, cache_b, first_all, second_all = lax.map(one_clip, (block_input, input_cache, middle_cache, cotangent))
    factor = 1.0 / jnp.sqrt(jnp.float32(CLIPS * FRAMES * H * W))
    first_weight_grad = lax.optimization_barrier(jnp.sum(first_all, axis=0)) * factor
    second_weight_grad = lax.optimization_barrier(jnp.sum(second_all, axis=0)) * factor
    return (grads, cache_a, cache_b, first_weight_grad, second_weight_grad)
```

```python
import functools
import math

import jax
import jax.numpy as jnp
from jax import lax
from jax.experimental import pallas as pl
from jax.experimental.pallas import tpu as pltpu
from jax.sharding import PartitionSpec as P

F32, BF16 = jnp.float32, jnp.bfloat16
MESH = pl.DeviceIdType.MESH
ROWS, PAIRS, OWN = 32, 17, 16
SPAN, HALF = PAIRS * 128, OWN * 128
FLAT = PAIRS * ROWS
KEEP = OWN * ROWS
TAPS = 27
ZLO, XS, CORES, YS = 4, 4, 2, 4
PLANE, LINE = XS * YS, ZLO * 2
SUMS = 28 * 64
PART = SUMS // CORES
PIECE = PART // PLANE


def widen(wide, weight):
    def step(k):
        kt, kr = k // 3, k % 3
        none = jnp.zeros((64, 64), BF16)
        taps = [none] + [weight[3 * k + kq] for kq in range(3)] + [none]
        columns = pl.ds(pl.multiple_of(128 * kr, 128), 128)
        for a in range(4):
            block = jnp.concatenate([taps[a + 1], taps[a]], axis=1)
            wide[pl.ds(pl.multiple_of(256 * kt + 64 * a, 64), 64), columns] = block

    loop(0, 9, step)


def widen_back(wide, weight):
    def step(k):
        kt, kr = k // 3, k % 3
        none = jnp.zeros((64, 64), BF16)
        taps = [none] + [weight[3 * (8 - k) + 2 - kq] for kq in range(3)] + [none]
        for b in range(2):
            rows = pl.ds(pl.multiple_of(128 * kr + 64 * b, 64), 64)
            for a in range(0, 4, 2):
                block = jnp.concatenate([taps[a + 1 - b], taps[a + 2 - b]], axis=1)
                wide[rows, pl.ds(pl.multiple_of(256 * kt + 64 * a, 128), 128)] = block

    loop(0, 9, step)


def silu_slope(value):
    logistic = jax.nn.sigmoid(value)
    return logistic * (1.0 + value * (1.0 - logistic))


def row_of(shape):
    return lax.broadcasted_iota(jnp.int32, shape, 0) % ROWS


def row_before(block):
    return jnp.where(row_of(block.shape) == 0, 0.0, pltpu.roll(block, 1, axis=0))


def row_after(block):
    return jnp.where(row_of(block.shape) == ROWS - 1, 0.0, pltpu.roll(block, block.shape[0] - 1, axis=0))


def half_shift(block):
    turn = pltpu.roll(block, 64, axis=1)
    none = jnp.zeros((ROWS, 128), F32)
    lane = lax.broadcasted_iota(jnp.int32, (FLAT + ROWS, 128), 1)
    return jnp.where(lane < 64, jnp.concatenate([none, turn], 0), jnp.concatenate([turn, none], 0)).astype(BF16)


def flat(ref, slot):
    return jnp.concatenate([ref[slot, :, 128 * l : 128 * l + 128] for l in range(PAIRS)], axis=0).astype(F32)


def conv(ref, slot, weight, back=True):
    parts = []
    for j in range(3):
        parts += [ref[slot + j, 0:FLAT, :], ref[slot + j, ROWS : FLAT + ROWS, :]]
    over = (((1,), (1 if back else 0,)), ((), ()))
    sums = lax.dot_general(jnp.concatenate(parts, axis=1), weight[...], over, preferred_element_type=F32)
    return sums[:, 128:256] + row_before(sums[:, 0:128]) + row_after(sums[:, 256:384])


def three_rows(ref, slot, block):
    ref[slot, 0] = row_after(block).astype(BF16)
    ref[slot, 1] = block.astype(BF16)
    ref[slot, 2] = row_before(block).astype(BF16)


def loop(low, high, step):
    def body(i, carry):
        step(i)
        return carry

    lax.fori_loop(low, high, body, 0)


def kernel(
    factor,
    x_hbm, icache_hbm, mcache_hbm, ct_hbm, weight1, weight2, bias,
    out, icg, mcg, grad1, grad2,
    x, ct, mc, acts, cts, mid3, slope, pg, pg3, pgs, eg, icp, mcp, raw1, raw2,
    w1, w2t, w1t, vsum, from_core, part, plane_out, plane_in, line, whole,
    core_sem, plane_send, plane_recv, line_send, line_recv, spread_send, spread_recv,
    local_sem, send_sem, recv_sem, piece_send, piece_recv, own_sem,
):
    tm = lax.axis_index("tm")
    four, side = tm // 2, tm % 2
    first, last = four == 0, four == 3
    other = tm + 1 - 2 * side
    clip = lax.axis_index("clip")
    zlo, across, core = clip // (XS * CORES), (clip // CORES) % XS, clip % CORES
    spot, depth = across * YS + four, zlo * 2 + side

    def in_plane(i):
        to = (spot + i) % PLANE
        return to, {"clip": (zlo * XS + to // YS) * CORES + core, "tm": to % YS * 2 + side}

    def in_line(i):
        to = (depth + i) % LINE
        return {"clip": (to // 2 * XS + across) * CORES + core, "tm": four * 2 + to % 2}

    def anyone(src, dst, send, recv, to):
        return pltpu.make_async_remote_copy(src, dst, send, recv, device_id=to, device_id_type=MESH)

    twin = {"clip": clip + 1 - 2 * core, "tm": tm}
    mine = pl.ds(pl.multiple_of(side * (15 * 128), 128), SPAN)
    theirs = pl.ds(pl.multiple_of((1 - side) * (15 * 128), 128), SPAN)
    keep = pl.ds(pl.multiple_of(side * 128, 128), HALF)
    home = pl.ds(pl.multiple_of(side * HALF, 128), HALF)

    def remote(src, dst, i, to):
        return pltpu.make_async_remote_copy(
            src, dst, send_sem.at[i], recv_sem.at[i], device_id={"tm": to}, device_id_type=MESH
        )

    here = []
    for f in range(2):
        here.append(pltpu.make_async_copy(x_hbm.at[f, :, mine], x.at[2 + 2 * side + f], local_sem.at[f]))
        here.append(pltpu.make_async_copy(ct_hbm.at[f, :, mine], ct.at[2 * side + f], local_sem.at[2 + f]))
    for copy in here:
        copy.start()
    cached = []
    for f in range(2):
        cached.append(pltpu.make_async_copy(icache_hbm.at[f, :, mine], x.at[f], local_sem.at[4 + f]))
        cached.append(pltpu.make_async_copy(mcache_hbm.at[f, :, mine], mc.at[f], local_sem.at[6 + f]))

    @pl.when(first)
    def _():
        for copy in cached:
            copy.start()

    barrier = pltpu.get_barrier_semaphore()
    for d in range(1, 8):
        pl.semaphore_signal(barrier, inc=1, device_id={"tm": (tm + d) % 8}, device_id_type=MESH)
    greeted = 8
    pl.semaphore_signal(barrier, inc=1, device_id=twin, device_id_type=MESH)
    for i in range(1, XS):
        for j in range(YS):
            to = {"clip": (zlo * XS + (across + i) % XS) * CORES + core, "tm": (four + j) % YS * 2 + side}
            pl.semaphore_signal(barrier, inc=1, device_id=to, device_id_type=MESH)
            greeted += 1
    for i in range(1, ZLO):
        for j in range(2):
            to = {"clip": ((zlo + i) % ZLO * XS + across) * CORES + core, "tm": four * 2 + (side + j) % 2}
            pl.semaphore_signal(barrier, inc=1, device_id=to, device_id_type=MESH)
            greeted += 1
    pl.semaphore_wait(barrier, greeted)

    x_swap = [remote(x_hbm.at[f, :, theirs], x.at[2 + 2 * side + f], f, other) for f in range(2)]
    ct_swap = [remote(ct_hbm.at[f, :, theirs], ct.at[2 * side + f], 2 + f, other) for f in range(2)]
    x_halo = [remote(x.at[4 + f], x.at[f], 4 + f, (tm + 2) % 8) for f in range(2)]
    ct_halo = [remote(ct.at[f], ct.at[4 + f], 6 + f, (tm + 6) % 8) for f in range(2)]
    pg_halo = [remote(pg.at[f], pg.at[4 + f], 8 + f, (tm + 6) % 8) for f in range(2)]
    for copy in x_swap + ct_swap:
        copy.start()
    for copy in here:
        copy.wait()

    @pl.when((side == 1) & jnp.logical_not(last))
    def _():
        for copy in x_halo:
            copy.start()

    @pl.when((side == 0) & jnp.logical_not(first))
    def _():
        for copy in ct_halo:
            copy.start()

    def activate(s):
        acts[s] = half_shift(jax.nn.silu(flat(x, s)))

    widen(w1, weight1)
    widen_back(w2t, weight2)
    widen_back(w1t, weight1)
    two_biases = jnp.concatenate([bias[...], bias[...]], axis=1)
    vsum[64 * TAPS :, :] = jnp.zeros((64, 128), F32)
    raw1[...] = jnp.zeros_like(raw1)
    raw2[...] = jnp.zeros_like(raw2)
    for s in range(2):
        cts[s] = jnp.zeros((FLAT + ROWS, 128), BF16)
        pgs[s] = jnp.zeros((FLAT + ROWS, 128), BF16)
    for f in range(2):
        x_swap[f].wait_recv()

        @pl.when((side == 0) & jnp.logical_not(last))
        def _():
            x_halo[f].start()

    loop(2, 6, activate)

    @pl.when(first)
    def _():
        for copy in cached:
            copy.wait()

    @pl.when(jnp.logical_not(first))
    def _():
        for copy in x_halo:
            copy.wait_recv()

    loop(0, 2, activate)

    def forward(t):
        pre = conv(acts, t, w1, False) + two_biases
        slope[t] = silu_slope(pre)
        three_rows(mid3, t + 2, jax.nn.silu(pre).astype(BF16).astype(F32))

    loop(0, 4, forward)

    @pl.when(first)
    def _():
        loop(0, 2, lambda s: three_rows(mid3, s, flat(mc, s)))

    for f in range(2):
        ct_swap[f].wait_recv()

        @pl.when((side == 1) & jnp.logical_not(first))
        def _():
            ct_halo[f].start()

    def shift_ct(s):
        cts[s + 2] = half_shift(flat(ct, s))

    def pre_gradient(n):
        grad = (conv(cts, n, w2t) * slope[n - 2]).astype(BF16)
        pg[n - 2] = grad
        grad = grad.astype(F32)
        three_rows(pg3, n - 2, grad)
        pgs[n] = half_shift(grad)

    loop(0, 4, shift_ct)
    loop(2, 4, pre_gradient)

    @pl.when(last)
    def _():
        for s in range(6, 8):
            cts[s] = jnp.zeros((FLAT + ROWS, 128), BF16)

    @pl.when(jnp.logical_not(last))
    def _():
        for copy in ct_halo:
            copy.wait_recv()
        loop(4, 6, shift_ct)

    @pl.when(jnp.logical_not(first))
    def _():
        for copy in pg_halo:
            copy.start()

    loop(4, 6, pre_gradient)

    def pieces(ref, f, block):
        wide = jnp.concatenate([block[ROWS * l : ROWS * l + ROWS, :] for l in range(PAIRS)], axis=1)
        for p in range(8):
            ref[p, f] = wide[4 * p : 4 * p + 4, :].astype(BF16)

    def deal(ref, result, k, start):
        for p in range(8):
            far = pltpu.make_async_remote_copy(
                ref.at[p, :, :, keep], result.at[:, :, home], piece_send.at[k, p], piece_recv.at[k, side],
                device_id={"tm": p}, device_id_type=MESH,
            )
            near = pltpu.make_async_copy(ref.at[p, :, :, keep], result.at[:, :, home], own_sem.at[k])

            @pl.when(first & (tm != p))
            def _():
                far.start() if start else far.wait_send()

            @pl.when(first & (tm == p))
            def _():
                near.start() if start else near.wait()

    def dealt(ref, result, k):
        for s in range(2):
            columns = pl.ds(s * HALF, HALF)

            @pl.when(tm != s)
            def _():
                pltpu.make_async_remote_copy(
                    ref.at[0, :, :, pl.ds(0, HALF)], result.at[:, :, columns], piece_send.at[k, 0], piece_recv.at[k, s],
                    device_id={"tm": tm}, device_id_type=MESH,
                ).wait_recv()

    @pl.when(first)
    def _():
        loop(0, 2, lambda n: pieces(mcp, n, conv(cts, n, w2t)))

    deal(mcp, mcg, 0, True)

    own = pl.ds(pl.multiple_of(side * ROWS, ROWS), KEEP)
    next_own = pl.ds(pl.multiple_of(side * ROWS + ROWS, ROWS), KEEP)

    def operands(still, still_slot, moved, moved_slot):
        one = jnp.concatenate([still[still_slot, v, own, :] for v in range(3)], axis=1)
        parts = []
        for j in range(3):
            parts += [moved[moved_slot + j, own, :], moved[moved_slot + j, next_own, :]]
        return one, jnp.concatenate(parts, axis=1)

    over_rows = (((0,), (0,)), ((), ()))

    def second_sum(n):
        one, four_px = operands(mid3, n, cts, n)
        raw2[...] += lax.dot_general(one, four_px, over_rows, preferred_element_type=F32)

    def first_sum(t):
        one, four_px = operands(pg3, t, acts, t)
        raw1[...] += lax.dot_general(four_px, one, over_rows, preferred_element_type=F32)

    loop(jnp.where(first, 0, 2), 6, second_sum)
    loop(0, 4, first_sum)
    lane = lax.broadcasted_iota(jnp.int32, (64, 128), 1)
    for kt in range(3):
        for kr in range(3):
            one = 128 * kr
            two = 128 * (2 - kr)
            low = raw2[two : two + 64, 256 * (2 - kt) : 256 * (3 - kt)]
            high = raw2[two + 64 : two + 128, 256 * (2 - kt) : 256 * (3 - kt)]
            second = low + pltpu.roll(high, 192, axis=1)
            for kq in range(3):
                at = 256 * kt + 64 * kq
                tap = (kt * 3 + kr) * 3 + kq
                left = raw1[at : at + 64, one : one + 128]
                left += pltpu.roll(raw1[at + 64 : at + 128, one : one + 128], 64, axis=1)
                right = second[:, 128 * ((2 - kq) // 2) : 128 * ((2 - kq) // 2) + 128]
                if kq != 1:
                    right = pltpu.roll(right, 64, axis=1)
                vsum[64 * tap : 64 * tap + 64, :] = jnp.where(lane < 64, left, right)

    half_of = lambda c: pl.ds(pl.multiple_of(c * PART, 8), PART)
    cores = anyone(vsum.at[half_of(1 - core)], from_core, core_sem.at[0], core_sem.at[1], twin)
    cores.start()

    @pl.when(last)
    def _():
        for s in range(6, 8):
            pgs[s] = jnp.zeros((FLAT + ROWS, 128), BF16)

    def shift_pg(s):
        pgs[s + 2] = half_shift(pg[s].astype(F32))

    @pl.when(jnp.logical_not(last))
    def _():
        for copy in pg_halo:
            copy.wait_recv()
        loop(4, 6, shift_pg)

    def extended_gradient(n):
        return conv(pgs, n, w1t) * silu_slope(flat(x, n))

    def input_gradient(i):
        t = (2 * (1 - side) + i) % 4
        block = extended_gradient(t + 2) + flat(ct, t)
        for l in range(PAIRS):
            eg[i, :, 128 * l : 128 * l + 128] = block[ROWS * l : ROWS * l + ROWS, :].astype(BF16)

    back = [remote(eg.at[f, :, keep], out.at[f, :, home], 10 + f, other) for f in range(2)]
    stay = [pltpu.make_async_copy(eg.at[2 + f, :, keep], out.at[f, :, home], local_sem.at[f]) for f in range(2)]
    loop(0, 1, input_gradient)
    cores.wait_recv()
    part[...] = vsum[half_of(core), :] + from_core[...]
    plane_out[...] = part[...].reshape(PLANE, PIECE, 128).astype(BF16)
    loop(1, 2, input_gradient)
    gathers = []
    for i in range(1, PLANE):
        to, device = in_plane(i)
        gathers.append(anyone(plane_out.at[to], plane_in.at[i], plane_send.at[i], plane_recv.at[i], device))
    for copy in gathers + back:
        copy.start()
    loop(2, 4, input_gradient)

    @pl.when(first)
    def _():
        loop(0, 2, lambda n: pieces(icp, n, extended_gradient(n)))

    for copy in stay:
        copy.start()
    total = part[pl.ds(pl.multiple_of(spot * PIECE, 8), PIECE), :]
    for i, copy in enumerate(gathers):
        copy.wait_recv()
        total += plane_in[i + 1].astype(F32)
    line[depth] = total.astype(BF16)
    deal(icp, icg, 1, True)
    lines = [anyone(line.at[depth], line.at[depth], line_send.at[i], line_recv.at[i], in_line(i)) for i in range(1, LINE)]
    for copy in lines:
        copy.start()
    for copy in lines:
        copy.wait_recv()
    total = line[0].astype(F32)
    for i in range(1, LINE):
        total += line[i].astype(F32)
    whole[core, spot] = (total * factor).astype(BF16)
    spreads = []
    for i in range(1, PLANE):
        to, device = in_plane(i)
        spreads.append(anyone(whole.at[core, spot], whole.at[core, spot], spread_send.at[i], spread_recv.at[i], device))
    for copy in spreads:
        copy.start()
    for copy in spreads:
        copy.wait_recv()
    twins = anyone(whole.at[core], whole.at[core], core_sem.at[2], core_sem.at[3], twin)
    twins.start()
    twins.wait_recv()
    sums = whole[...].astype(F32).reshape(SUMS, 128)
    for tap in range(TAPS):
        block = sums[64 * tap : 64 * tap + 64, :]
        grad1[tap] = block[:, 0:64]
        grad2[tap] = pltpu.roll(block, 64, axis=1)[:, 0:64]

    for copy in stay:
        copy.wait()
    for copy in x_swap + ct_swap + [cores, twins] + gathers + lines + spreads:
        copy.wait_send()

    @pl.when(jnp.logical_not(last))
    def _():
        for copy in x_halo:
            copy.wait_send()

    @pl.when(jnp.logical_not(first))
    def _():
        for copy in ct_halo + pg_halo:
            copy.wait_send()

    for copy in back:
        copy.wait()
    deal(mcp, mcg, 0, False)
    deal(icp, icg, 1, False)
    dealt(mcp, mcg, 0)
    dealt(icp, icg, 1)


def body(block_input, input_cache, middle_cache, first_weight, first_bias, second_weight, cotangent):
    count = 1024 * lax.axis_size("clip") * lax.axis_size("tm") * 4
    anywhere = pl.BlockSpec(memory_space=pl.ANY)
    inside = pl.BlockSpec(memory_space=pltpu.VMEM)
    out, icg, mcg, grad1, grad2 = pl.pallas_call(
        functools.partial(kernel, 1.0 / math.sqrt(count)),
        out_shape=(
            jax.ShapeDtypeStruct((2, ROWS, 4096), BF16),
            jax.ShapeDtypeStruct((2, 4, 4096), BF16),
            jax.ShapeDtypeStruct((2, 4, 4096), BF16),
            jax.ShapeDtypeStruct((TAPS, 64, 64), F32),
            jax.ShapeDtypeStruct((TAPS, 64, 64), F32),
        ),
        in_specs=[anywhere] * 4 + [inside] * 3,
        out_specs=(anywhere, anywhere, anywhere, inside, inside),
        scratch_shapes=[
            pltpu.VMEM((6, ROWS, SPAN), BF16),
            pltpu.VMEM((6, ROWS, SPAN), BF16),
            pltpu.VMEM((2, ROWS, SPAN), BF16),
            pltpu.VMEM((6, FLAT + ROWS, 128), BF16),
            pltpu.VMEM((8, FLAT + ROWS, 128), BF16),
            pltpu.VMEM((6, 3, FLAT, 128), BF16),
            pltpu.VMEM((4, FLAT, 128), F32),
            pltpu.VMEM((6, FLAT, 128), BF16),
            pltpu.VMEM((4, 3, FLAT, 128), BF16),
            pltpu.VMEM((8, FLAT + ROWS, 128), BF16),
            pltpu.VMEM((4, ROWS, SPAN), BF16),
            pltpu.VMEM((8, 2, 4, SPAN), BF16),
            pltpu.VMEM((8, 2, 4, SPAN), BF16),
            pltpu.VMEM((768, 384), F32),
            pltpu.VMEM((384, 768), F32),
            pltpu.VMEM((768, 384), BF16),
            pltpu.VMEM((384, 768), BF16),
            pltpu.VMEM((384, 768), BF16),
            pltpu.VMEM((SUMS, 128), F32),
            pltpu.VMEM((PART, 128), F32),
            pltpu.VMEM((PART, 128), F32),
            pltpu.VMEM((PLANE, PIECE, 128), BF16),
            pltpu.VMEM((PLANE, PIECE, 128), BF16),
            pltpu.VMEM((LINE, PIECE, 128), BF16),
            pltpu.VMEM((CORES, PLANE, PIECE, 128), BF16),
            pltpu.SemaphoreType.DMA((4,)),
            pltpu.SemaphoreType.DMA((PLANE,)),
            pltpu.SemaphoreType.DMA((PLANE,)),
            pltpu.SemaphoreType.DMA((LINE,)),
            pltpu.SemaphoreType.DMA((LINE,)),
            pltpu.SemaphoreType.DMA((PLANE,)),
            pltpu.SemaphoreType.DMA((PLANE,)),
            pltpu.SemaphoreType.DMA((8,)),
            pltpu.SemaphoreType.DMA((12,)),
            pltpu.SemaphoreType.DMA((12,)),
            pltpu.SemaphoreType.DMA((2, 8)),
            pltpu.SemaphoreType.DMA((2, 2)),
            pltpu.SemaphoreType.DMA((2,)),
        ],
        compiler_params=pltpu.CompilerParams(
            collective_id=0, has_side_effects=True, vmem_limit_bytes=56 << 20
        ),
    )(
        block_input[0], input_cache[0], middle_cache[0], cotangent[0],
        first_weight.reshape(TAPS, 64, 64), second_weight.reshape(TAPS, 64, 64), first_bias.reshape(1, 64),
    )
    shape = (3, 3, 3, 64, 64)
    return (out[None], icg[None], mcg[None], grad1.reshape(shape), grad2.reshape(shape))


def solution(mesh):
    return jax.shard_map(
        body,
        mesh=mesh,
        in_specs=(
            P("clip", "tm", None, None),
            P("clip", None, None, None),
            P("clip", None, None, None),
            P(),
            P(),
            P(),
            P("clip", "tm", None, None),
        ),
        out_specs=(
            P("clip", "tm", None, None),
            P("clip", None, "tm", None),
            P("clip", None, "tm", None),
            P(),
            P(),
        ),
        check_vma=False,
    )
```

```python
import functools
import math

import jax
import jax.numpy as jnp
from jax import lax
from jax.experimental import pallas as pl
from jax.experimental.pallas import tpu as pltpu
from jax.sharding import PartitionSpec as P

F32, BF16 = jnp.float32, jnp.bfloat16
MESH = pl.DeviceIdType.MESH
ROWS, PAIRS, OWN = 32, 17, 16
SPAN, HALF = PAIRS * 128, OWN * 128
FLAT = PAIRS * ROWS
KEEP = OWN * ROWS
TAPS = 27
ARRIVE = ((0, 5), (5, 9), (9, 13), (13, 17))
FOLLOW = ((0, 4), (4, 8), (8, 12), (12, 17))
SETTLE = ((0, 3), (3, 7), (7, 11), (11, 16))
ZLO, XS, CORES, YS = 4, 4, 2, 4
PLANE, LINE = XS * YS, ZLO * 2
SUMS = 28 * 64
PART = SUMS // CORES
PIECE = PART // PLANE


def widen(wide, weight):
    def step(k):
        kt, kr = k // 3, k % 3
        none = jnp.zeros((64, 64), BF16)
        taps = [none] + [weight[3 * k + kq] for kq in range(3)] + [none]
        columns = pl.ds(pl.multiple_of(128 * kr, 128), 128)
        for a in range(4):
            block = jnp.concatenate([taps[a + 1], taps[a]], axis=1)
            wide[pl.ds(pl.multiple_of(256 * kt + 64 * a, 64), 64), columns] = block

    loop(0, 9, step)


def widen_back(wide, weight):
    def step(k):
        kt, kr = k // 3, k % 3
        none = jnp.zeros((64, 64), BF16)
        taps = [none] + [weight[3 * (8 - k) + 2 - kq] for kq in range(3)] + [none]
        for b in range(2):
            rows = pl.ds(pl.multiple_of(128 * kr + 64 * b, 64), 64)
            for a in range(0, 4, 2):
                block = jnp.concatenate([taps[a + 1 - b], taps[a + 2 - b]], axis=1)
                wide[rows, pl.ds(pl.multiple_of(256 * kt + 64 * a, 128), 128)] = block

    loop(0, 9, step)


def silu_slope(value):
    logistic = jax.nn.sigmoid(value)
    return logistic * (1.0 + value * (1.0 - logistic))


def row_of(shape):
    return lax.broadcasted_iota(jnp.int32, shape, 0) % ROWS


def row_before(block):
    return jnp.where(row_of(block.shape) == 0, 0.0, pltpu.roll(block, 1, axis=0))


def row_after(block):
    return jnp.where(row_of(block.shape) == ROWS - 1, 0.0, pltpu.roll(block, block.shape[0] - 1, axis=0))


def half_shift(block, ends=True):
    none = jnp.zeros((ROWS, 128), F32)
    turn = pltpu.roll(block, 64, axis=1)
    left, right = (jnp.concatenate([none, turn], 0), jnp.concatenate([turn, none], 0)) if ends else (turn[:-ROWS], turn[ROWS:])
    lane = lax.broadcasted_iota(jnp.int32, left.shape, 1)
    return jnp.where(lane < 64, left, right).astype(BF16)


def piece_shift(load, low, high):
    none = jnp.zeros((ROWS, 128), F32)
    blocks = [load(l).astype(F32) if 0 <= l < PAIRS else none for l in range(low - 1, high + (high == PAIRS))]
    return half_shift(jnp.concatenate(blocks, 0), False)


def flat(ref, slot):
    return jnp.concatenate([ref[slot, :, 128 * l : 128 * l + 128] for l in range(PAIRS)], axis=0).astype(F32)


def conv(ref, slots, weight, back=True, low=0, high=PAIRS):
    frames = []
    for slot in slots:
        parts = []
        for j in range(3):
            parts += [ref[slot + j, ROWS * low : ROWS * high, :], ref[slot + j, ROWS * low + ROWS : ROWS * high + ROWS, :]]
        frames.append(jnp.concatenate(parts, axis=1))
    over = (((1,), (1 if back else 0,)), ((), ()))
    sums = lax.dot_general(jnp.concatenate(frames, axis=0), weight[...], over, preferred_element_type=F32)
    return sums[:, 128:256] + row_before(sums[:, 0:128]) + row_after(sums[:, 256:384])


def three_rows(ref, slot, block):
    ref[slot, 0] = row_after(block).astype(BF16)
    ref[slot, 1] = block.astype(BF16)
    ref[slot, 2] = row_before(block).astype(BF16)


def loop(low, high, step):
    def body(i, carry):
        step(i)
        return carry

    lax.fori_loop(low, high, body, 0)


def kernel(
    factor,
    x_hbm, icache_hbm, mcache_hbm, ct_hbm, weight1, weight2, bias,
    out, icg, mcg, sums,
    x, ct, mc, acts, cts, mid3, slope, mid_grad, pg, pg3, pgs, eg, dealt, passed, raw1, raw2,
    w1, w2t, w1t, vsum, from_core, plane_out, plane_in, line, whole,
    core_sem, plane_send, plane_recv, line_send, line_recv, spread_send, spread_recv, leave_sem,
    local_sem, send_sem, recv_sem, deal_sem, pass_send, pass_recv, own_sem,
):
    tm = lax.axis_index("tm")
    four, side = tm // 2, tm % 2
    first, last = four == 0, four == 3
    other = tm + 1 - 2 * side
    clip = lax.axis_index("clip")
    zlo, across, core = clip // (XS * CORES), (clip // CORES) % XS, clip % CORES
    spot, depth = across * YS + four, zlo * 2 + side

    def in_plane(i):
        to = (spot + i) % PLANE
        return to, {"clip": (zlo * XS + to // YS) * CORES + core, "tm": to % YS * 2 + side}

    def in_line(i):
        to = (depth + i) % LINE
        return {"clip": (to // 2 * XS + across) * CORES + core, "tm": four * 2 + to % 2}

    def anyone(src, dst, send, recv, to):
        return pltpu.make_async_remote_copy(src, dst, send, recv, device_id=to, device_id_type=MESH)

    twin = {"clip": clip + 1 - 2 * core, "tm": tm}
    mine = pl.ds(pl.multiple_of(side * (15 * 128), 128), SPAN)
    theirs = pl.ds(pl.multiple_of((1 - side) * (15 * 128), 128), SPAN)
    keep = pl.ds(pl.multiple_of(side * 128, 128), HALF)
    home = pl.ds(pl.multiple_of(side * HALF, 128), HALF)

    def remote(src, dst, i, to):
        return pltpu.make_async_remote_copy(
            src, dst, send_sem.at[i], recv_sem.at[i], device_id={"tm": to}, device_id_type=MESH
        )

    here = []
    for f in range(2):
        here.append(pltpu.make_async_copy(x_hbm.at[f, :, mine], x.at[2 + 2 * side + f], local_sem.at[f]))
        here.append(pltpu.make_async_copy(ct_hbm.at[f, :, mine], ct.at[2 * side + f], local_sem.at[2 + f]))
    for copy in here:
        copy.start()
    cached = []
    for f in range(2):
        cached.append(pltpu.make_async_copy(icache_hbm.at[f, :, mine], x.at[f], local_sem.at[4 + f]))
        cached.append(pltpu.make_async_copy(mcache_hbm.at[f, :, mine], mc.at[f], local_sem.at[6 + f]))

    @pl.when(first)
    def _():
        for copy in cached:
            copy.start()

    barrier = pltpu.get_barrier_semaphore()
    for d in range(1, 8):
        pl.semaphore_signal(barrier, inc=1, device_id={"tm": (tm + d) % 8}, device_id_type=MESH)
    greeted = 8
    pl.semaphore_signal(barrier, inc=1, device_id=twin, device_id_type=MESH)
    for i in range(1, XS):
        for j in range(YS):
            to = {"clip": (zlo * XS + (across + i) % XS) * CORES + core, "tm": (four + j) % YS * 2 + side}
            pl.semaphore_signal(barrier, inc=1, device_id=to, device_id_type=MESH)
            greeted += 1
    for i in range(1, ZLO):
        for j in range(2):
            to = {"clip": ((zlo + i) % ZLO * XS + across) * CORES + core, "tm": four * 2 + (side + j) % 2}
            pl.semaphore_signal(barrier, inc=1, device_id=to, device_id_type=MESH)
            greeted += 1
    pl.semaphore_wait(barrier, greeted)

    x_swap, ct_swap, x_halo, ct_halo, pg_halo = [], [], [], [], []
    for c, ((low, high), (a, b)) in enumerate(zip(ARRIVE, FOLLOW)):
        cut = pl.ds(pl.multiple_of((1 - side) * (15 * 128) + 128 * low, 128), 128 * (high - low))
        cols = pl.ds(128 * low, 128 * (high - low))
        rows = pl.ds(ROWS * a, ROWS * (b - a))
        ours, two, four_on = pl.ds(2 * side, 2), pl.ds(0, 2), pl.ds(4, 2)
        x_swap.append(remote(x_hbm.at[:, :, cut], x.at[pl.ds(2 + 2 * side, 2), :, cols], c, other))
        ct_swap.append(remote(ct_hbm.at[:, :, cut], ct.at[ours, :, cols], 4 + c, other))
        x_halo.append(remote(x.at[four_on, :, cols], x.at[two, :, cols], 8 + c, (tm + 2) % 8))
        ct_halo.append(remote(ct.at[two, :, cols], ct.at[four_on, :, cols], 12 + c, (tm + 6) % 8))
        pg_halo.append(remote(pg.at[two, rows, :], pg.at[four_on, rows, :], 16 + c, (tm + 6) % 8))

    @pl.when(side == 0)
    def _():
        for copy in ct_swap + x_swap:
            copy.start()

    @pl.when(side == 1)
    def _():
        for copy in x_swap + ct_swap:
            copy.start()

    for copy in here:
        copy.wait()

    @pl.when((side == 1) & jnp.logical_not(last))
    def _():
        for copy in x_halo:
            copy.start()

    @pl.when((side == 0) & jnp.logical_not(first))
    def _():
        for copy in ct_halo:
            copy.start()

    widen(w1, weight1)
    widen_back(w2t, weight2)
    widen_back(w1t, weight1)
    two_biases = jnp.concatenate([bias[...], bias[...]], axis=1)
    vsum[64 * TAPS :, :] = jnp.zeros((64, 128), F32)

    @pl.when(last)
    def _():
        for s in range(4, 6):
            ct[s] = jnp.zeros((ROWS, SPAN), BF16)
            pg[s] = jnp.zeros((FLAT, 128), BF16)

    for s in range(2):
        cts[s] = jnp.zeros((FLAT + ROWS, 128), BF16)
        pgs[s] = jnp.zeros((FLAT + ROWS, 128), BF16)
    raw2[...] = jnp.zeros_like(raw2)

    def forward(c):
        @pl.when(jnp.logical_not(first))
        def _():
            x_halo[c].wait_recv()

        (low, high), (a, b) = ARRIVE[c], FOLLOW[c]
        for s in range(6):
            acts[s, ROWS * low : ROWS * (high + (high == PAIRS)), :] = piece_shift(
                lambda l, s=s: jax.nn.silu(x[s, :, 128 * l : 128 * l + 128].astype(F32)), low, high
            )
        pre = conv(acts, range(4), w1, False, a, b) + two_biases
        slopes = silu_slope(pre)
        middle = jax.nn.silu(pre).astype(BF16)
        wide = middle.astype(F32)
        before, after = row_before(wide).astype(BF16), row_after(wide).astype(BF16)
        size = ROWS * (b - a)
        for t in range(4):
            here, there = slice(size * t, size * t + size), slice(ROWS * a, ROWS * b)
            slope[t, there, :] = slopes[here]
            mid3[t + 2, 0, there, :] = after[here]
            mid3[t + 2, 1, there, :] = middle[here]
            mid3[t + 2, 2, there, :] = before[here]

    over_rows = (((0,), (0,)), ((), ()))

    def operands(still, moved, frames, ahead, rows):
        one, four_px = [], []
        for n in frames:
            one.append(jnp.concatenate([still[n, v, rows[0], :] for v in range(3)], axis=1))
            four_px.append(jnp.concatenate([moved[n + ahead + j, r, :] for j in range(3) for r in rows], axis=1))
        return jnp.concatenate(one, axis=0), jnp.concatenate(four_px, axis=0)

    def own_rows(c):
        i, k = SETTLE[c]
        return [pl.ds(pl.multiple_of((side + e + i) * ROWS, ROWS), ROWS * (k - i)) for e in range(2)]

    def backward(c):
        @pl.when(jnp.logical_not(last))
        def _():
            ct_halo[c].wait_recv()

        (low, high), (a, b) = ARRIVE[c], FOLLOW[c]
        for s in range(6):
            cts[s + 2, ROWS * low : ROWS * (high + (high == PAIRS)), :] = piece_shift(
                lambda l, s=s: ct[s, :, 128 * l : 128 * l + 128], low, high
            )
        grad = conv(cts, range(2, 6), w2t, low=a, high=b)
        size = ROWS * (b - a)
        for t in range(4):
            mid_grad[t, ROWS * a : ROWS * b, :] = grad[size * t : size * t + size]

        @pl.when(first)
        def _():
            one, four_px = operands(mid3, cts, range(2), 0, own_rows(c))
            raw2[...] += lax.dot_general(one, four_px, over_rows, preferred_element_type=F32)

    def settle(c):
        a, b = FOLLOW[c]
        size = ROWS * (b - a)
        grad = jnp.concatenate([mid_grad[t, ROWS * a : ROWS * b, :] for t in range(4)], axis=0)
        grad = (grad * jnp.concatenate([slope[t, ROWS * a : ROWS * b, :] for t in range(4)], axis=0)).astype(BF16)
        wide = grad.astype(F32)
        before, after = row_before(wide).astype(BF16), row_after(wide).astype(BF16)
        for t in range(4):
            here, there = slice(size * t, size * t + size), slice(ROWS * a, ROWS * b)
            pg[t, there, :] = grad[here]
            pg3[t, 0, there, :] = after[here]
            pg3[t, 1, there, :] = grad[here]
            pg3[t, 2, there, :] = before[here]
            pgs[t + 2, ROWS * a : ROWS * (b + (b == PAIRS)), :] = piece_shift(
                lambda l, t=t: pg[t, ROWS * l : ROWS * l + ROWS, :], a, b
            )
        rows = own_rows(c)
        raw2[...] += lax.dot_general(*operands(mid3, cts, range(2, 6), 0, rows), over_rows, preferred_element_type=F32)
        one, four_px = operands(pg3, acts, range(4), 0, rows)
        sums = lax.dot_general(four_px, one, over_rows, preferred_element_type=F32)
        raw1[...] = sums if c == 0 else raw1[...] + sums

        @pl.when(jnp.logical_not(first))
        def _():
            pg_halo[c].start()

    @pl.when(first)
    def _():
        for copy in cached:
            copy.wait()
        loop(0, 2, lambda s: three_rows(mid3, s, flat(mc, s)))

    @pl.when(side == 0)
    def _():
        for c in range(5):
            if c < 4:
                x_swap[c].wait_recv()

                @pl.when(jnp.logical_not(last))
                def _():
                    x_halo[c].start()

            if c > 0:
                forward(c - 1)

    @pl.when(side == 1)
    def _():
        for c in range(5):
            if c < 4:
                ct_swap[c].wait_recv()

                @pl.when(jnp.logical_not(first))
                def _():
                    ct_halo[c].start()

            if c > 0:
                backward(c - 1)

    for c in range(4):
        @pl.when(side == 0)
        def _():
            ct_swap[c].wait_recv()
            backward(c)

        @pl.when(side == 1)
        def _():
            x_swap[c].wait_recv()
            forward(c)

        settle(c)

    def pieces(k, f, block):
        wide = jnp.concatenate([block[ROWS * l : ROWS * l + ROWS, :] for l in range(PAIRS)], axis=1)
        for p in range(8):
            dealt[p, k, f] = wide[4 * p : 4 * p + 4, :].astype(BF16)

    deals = []
    for v in range(1, YS):
        pair = dealt.at[pl.ds(2 * v, 2), :, :, :, keep]
        deals.append(anyone(pair, passed, deal_sem.at[v], deal_sem.at[0], {"tm": 2 * v + side}))

    def pass_on(held, act):
        for k, result in enumerate((mcg, icg)):
            to = result.at[:, :, home]
            near = pltpu.make_async_copy(held(side, k), to, own_sem.at[k])
            act(near, anyone(held(1 - side, k), to, pass_send.at[k], pass_recv.at[k], {"tm": other}))

    def pass_all(act):
        @pl.when(first)
        def _():
            pass_on(lambda q, k: dealt.at[q, k, :, :, keep], act)

        @pl.when(jnp.logical_not(first))
        def _():
            pass_on(lambda q, k: passed.at[q, k], act)

    def extended_gradient(n):
        return conv(pgs, [n], w1t) * silu_slope(flat(x, n))

    def input_gradient(t):
        block = extended_gradient(t + 2) + flat(ct, t)
        for l in range(PAIRS):
            eg[t, :, 128 * l : 128 * l + 128] = block[ROWS * l : ROWS * l + ROWS, :].astype(BF16)

    far = 2 - 2 * side
    back = [remote(eg.at[far + f, :, keep], out.at[f, :, home], 20 + f, other) for f in range(2)]
    stay = [pltpu.make_async_copy(eg.at[2 - far + f, :, keep], out.at[f, :, home], local_sem.at[f]) for f in range(2)]
    lane = lax.broadcasted_iota(jnp.int32, (64, 128), 1)

    def fold(taps):
        for tap in taps:
            kt, kr, kq = tap // 9, tap // 3 % 3, tap % 3
            at, one, two = 256 * kt + 64 * kq, 128 * kr, 128 * (2 - kr)
            left = raw1[at : at + 64, one : one + 128]
            left += pltpu.roll(raw1[at + 64 : at + 128, one : one + 128], 64, axis=1)
            at = 256 * (2 - kt)
            low, high = raw2[two : two + 64, at : at + 256], raw2[two + 64 : two + 128, at : at + 256]
            if kq == 1:
                right = low[:, 0:128] + pltpu.roll(high[:, 128:256], 64, axis=1)
            else:
                tile = 1 - kq // 2
                right = pltpu.roll(low[:, 128 * tile : 128 * tile + 128], 64, axis=1) + high[:, 128 * tile : 128 * tile + 128]
            vsum[64 * tap : 64 * tap + 64, :] = jnp.where(lane < 64, left, right)

    half_of = lambda c: pl.ds(pl.multiple_of(c * PART, 8), PART)
    cores = anyone(vsum.at[half_of(1 - core)], from_core, core_sem.at[0], core_sem.at[1], twin)
    for k in range(2):

        @pl.when(core == k)
        def _():
            fold(range(14 * (1 - k), min(TAPS, 28 - 14 * k)))
            cores.start()
            fold(range(14 * k, min(TAPS, 14 + 14 * k)))


    loop(0, 2, input_gradient)

    @pl.when(side == 1)
    def _():
        for copy in back:
            copy.start()

    cores.wait_recv()

    def part(to):
        own = pl.ds(pl.multiple_of(core * PART + to * PIECE, 8), PIECE)
        return vsum[own, :] + from_core[pl.ds(pl.multiple_of(to * PIECE, 8), PIECE), :]

    gathers = []
    for i in range(1, PLANE):
        to, device = in_plane(i)
        plane_out[i] = part(to).astype(BF16)
        gathers.append(anyone(plane_out.at[i], plane_in.at[i], plane_send.at[i], plane_recv.at[i], device))
        gathers[-1].start()
    @pl.when(jnp.logical_not(last))
    def _():
        for copy in pg_halo:
            copy.wait_recv()

    def shift_pg(s):
        pgs[s + 2] = half_shift(pg[s].astype(F32))

    loop(4, 6, shift_pg)
    loop(2, 3, input_gradient)

    @pl.when(side == 0)
    def _():
        back[0].start()

    loop(3, 4, input_gradient)

    @pl.when(side == 0)
    def _():
        back[1].start()

    for copy in stay:
        copy.start()
    @pl.when(first)
    def _():
        loop(0, 2, lambda n: pieces(0, n, conv(cts, [n], w2t)))
        loop(0, 2, lambda n: pieces(1, n, extended_gradient(n)))
        for copy in deals:
            copy.start()

    total = part(spot)
    for i, copy in enumerate(gathers):
        copy.wait_recv()
        total += plane_in[i + 1].astype(F32)
    line[depth] = total.astype(BF16)
    lines = [anyone(line.at[depth], line.at[depth], line_send.at[i], line_recv.at[i], in_line(i)) for i in range(1, LINE)]
    for copy in lines:
        copy.start()
    for copy in lines:
        copy.wait_recv()
    total = line[0].astype(F32)
    for i in range(1, LINE):
        total += line[i].astype(F32)
    whole[core, spot] = (total * factor).astype(BF16)
    spreads = []
    for i in range(1, PLANE):
        to, device = in_plane(i)
        spreads.append(anyone(whole.at[core, spot], whole.at[core, spot], spread_send.at[i], spread_recv.at[i], device))
    for copy in spreads:
        copy.start()

    @pl.when(jnp.logical_not(first))
    def _():
        deals[0].wait_recv()

    pass_all(lambda near, far: (near.start(), far.start()))
    for copy in spreads:
        copy.wait_recv()
    twins = anyone(whole.at[core], whole.at[core], core_sem.at[2], core_sem.at[3], twin)
    twins.start()
    leave = [pltpu.make_async_copy(whole.at[h], sums.at[h], leave_sem.at[e]) for e, h in enumerate((core, 1 - core))]
    leave[0].start()
    twins.wait_recv()
    leave[1].start()
    for copy in stay:
        copy.wait()
    for copy in x_swap + ct_swap + [cores, twins] + gathers + lines + spreads:
        copy.wait_send()

    @pl.when(jnp.logical_not(last))
    def _():
        for copy in x_halo:
            copy.wait_send()

    @pl.when(jnp.logical_not(first))
    def _():
        for copy in ct_halo + pg_halo:
            copy.wait_send()

    back[0].wait_recv()
    back[1].wait_recv()
    for copy in back:
        copy.wait_send()
    @pl.when(first)
    def _():
        for copy in deals:
            copy.wait_send()

    for copy in leave:
        copy.wait()
    pass_all(lambda near, far: (near.wait(), far.wait()))


def deliver(
    out_in, icg_in, mcg_in, sums_in, out, icg, mcg, grad1, grad2, out_at, icg_at, mcg_at, sums_at, one, two, in_sem, out_sem
):
    loads = [
        pltpu.make_async_copy(src, dst, in_sem.at[i])
        for i, (src, dst) in enumerate(((sums_in, sums_at), (out_in, out_at), (icg_in, icg_at), (mcg_in, mcg_at)))
    ]
    stores = [
        pltpu.make_async_copy(src, dst, out_sem.at[i])
        for i, (src, dst) in enumerate(((out_at, out), (icg_at, icg), (mcg_at, mcg)))
    ]
    for copy in loads:
        copy.start()
    loads[0].wait()
    for k in range(3):
        part = pl.ds(9 * k, 9)
        block = sums_at[...].astype(F32).reshape(SUMS, 128)[576 * k : 576 * k + 576]
        turned_block = pltpu.roll(block, 64, axis=1)
        for tap in range(9):
            one[9 * k + tap] = block[64 * tap : 64 * tap + 64, 0:64]
            two[9 * k + tap] = turned_block[64 * tap : 64 * tap + 64, 0:64]
        stores.append(pltpu.make_async_copy(one.at[part], grad1.at[part], out_sem.at[3 + 2 * k]))
        stores.append(pltpu.make_async_copy(two.at[part], grad2.at[part], out_sem.at[4 + 2 * k]))
        for copy in stores[-2:]:
            copy.start()
    for load, store in zip(loads[1:], stores[:3]):
        load.wait()
        store.start()
    for copy in stores:
        copy.wait()


def body(block_input, input_cache, middle_cache, first_weight, first_bias, second_weight, cotangent):
    count = 1024 * lax.axis_size("clip") * lax.axis_size("tm") * 4
    anywhere = pl.BlockSpec(memory_space=pl.ANY)
    inside = pl.BlockSpec(memory_space=pltpu.VMEM)
    results = pl.pallas_call(
        functools.partial(kernel, 1.0 / math.sqrt(count)),
        out_shape=(
            jax.ShapeDtypeStruct((2, ROWS, 4096), BF16),
            jax.ShapeDtypeStruct((2, 4, 4096), BF16),
            jax.ShapeDtypeStruct((2, 4, 4096), BF16),
            jax.ShapeDtypeStruct((CORES, PLANE, PIECE, 128), BF16),
        ),
        in_specs=[anywhere] * 4 + [inside] * 3,
        out_specs=(anywhere,) * 4,
        scratch_shapes=[
            pltpu.VMEM((6, ROWS, SPAN), BF16),
            pltpu.VMEM((6, ROWS, SPAN), BF16),
            pltpu.VMEM((2, ROWS, SPAN), BF16),
            pltpu.VMEM((6, FLAT + ROWS, 128), BF16),
            pltpu.VMEM((8, FLAT + ROWS, 128), BF16),
            pltpu.VMEM((6, 3, FLAT, 128), BF16),
            pltpu.VMEM((4, FLAT, 128), F32),
            pltpu.VMEM((4, FLAT, 128), F32),
            pltpu.VMEM((6, FLAT, 128), BF16),
            pltpu.VMEM((4, 3, FLAT, 128), BF16),
            pltpu.VMEM((8, FLAT + ROWS, 128), BF16),
            pltpu.VMEM((4, ROWS, SPAN), BF16),
            pltpu.VMEM((8, 2, 2, 4, SPAN), BF16),
            pltpu.VMEM((2, 2, 2, 4, HALF), BF16),
            pltpu.VMEM((768, 384), F32),
            pltpu.VMEM((384, 768), F32),
            pltpu.VMEM((768, 384), BF16),
            pltpu.VMEM((384, 768), BF16),
            pltpu.VMEM((384, 768), BF16),
            pltpu.VMEM((SUMS, 128), F32),
            pltpu.VMEM((PART, 128), F32),
            pltpu.VMEM((PLANE, PIECE, 128), BF16),
            pltpu.VMEM((PLANE, PIECE, 128), BF16),
            pltpu.VMEM((LINE, PIECE, 128), BF16),
            pltpu.VMEM((CORES, PLANE, PIECE, 128), BF16),
            pltpu.SemaphoreType.DMA((4,)),
            pltpu.SemaphoreType.DMA((PLANE,)),
            pltpu.SemaphoreType.DMA((PLANE,)),
            pltpu.SemaphoreType.DMA((LINE,)),
            pltpu.SemaphoreType.DMA((LINE,)),
            pltpu.SemaphoreType.DMA((PLANE,)),
            pltpu.SemaphoreType.DMA((PLANE,)),
            pltpu.SemaphoreType.DMA((2,)),
            pltpu.SemaphoreType.DMA((8,)),
            pltpu.SemaphoreType.DMA((22,)),
            pltpu.SemaphoreType.DMA((22,)),
            pltpu.SemaphoreType.DMA((YS,)),
            pltpu.SemaphoreType.DMA((2,)),
            pltpu.SemaphoreType.DMA((2,)),
            pltpu.SemaphoreType.DMA((2,)),
        ],
        compiler_params=pltpu.CompilerParams(
            collective_id=0, has_side_effects=True, vmem_limit_bytes=56 << 20
        ),
    )(
        block_input[0], input_cache[0], middle_cache[0], cotangent[0],
        first_weight.reshape(TAPS, 64, 64), second_weight.reshape(TAPS, 64, 64), first_bias.reshape(1, 64),
    )
    out, icg, mcg, grad1, grad2 = pl.pallas_call(
        deliver,
        out_shape=(
            jax.ShapeDtypeStruct((2, ROWS, 4096), BF16),
            jax.ShapeDtypeStruct((2, 4, 4096), BF16),
            jax.ShapeDtypeStruct((2, 4, 4096), BF16),
            jax.ShapeDtypeStruct((TAPS, 64, 64), F32),
            jax.ShapeDtypeStruct((TAPS, 64, 64), F32),
        ),
        in_specs=[anywhere] * 4,
        out_specs=(anywhere,) * 5,
        scratch_shapes=[
            pltpu.VMEM((2, ROWS, 4096), BF16),
            pltpu.VMEM((2, 4, 4096), BF16),
            pltpu.VMEM((2, 4, 4096), BF16),
            pltpu.VMEM((CORES, PLANE, PIECE, 128), BF16),
            pltpu.VMEM((TAPS, 64, 64), F32),
            pltpu.VMEM((TAPS, 64, 64), F32),
            pltpu.SemaphoreType.DMA((4,)),
            pltpu.SemaphoreType.DMA((9,)),
        ],
    )(*results)
    shape = (3, 3, 3, 64, 64)
    return (out[None], icg[None], mcg[None], grad1.reshape(shape), grad2.reshape(shape))


def solution(mesh):
    return jax.shard_map(
        body,
        mesh=mesh,
        in_specs=(
            P("clip", "tm", None, None),
            P("clip", None, None, None),
            P("clip", None, None, None),
            P(),
            P(),
            P(),
            P("clip", "tm", None, None),
        ),
        out_specs=(
            P("clip", "tm", None, None),
            P("clip", None, "tm", None),
            P("clip", None, "tm", None),
            P(),
            P(),
        ),
        check_vma=False,
    )
```

```python
import functools
import math

import jax
import jax.numpy as jnp
from jax import lax
from jax.experimental import pallas as pl
from jax.experimental.pallas import tpu as pltpu
from jax.sharding import PartitionSpec as P

F32, BF16 = jnp.float32, jnp.bfloat16
MESH = pl.DeviceIdType.MESH
ROWS, PAIRS, OWN = 32, 17, 16
SPAN, HALF = PAIRS * 128, OWN * 128
FLAT = PAIRS * ROWS
KEEP = OWN * ROWS
TAPS = 27
ARRIVE = ((0, 5), (5, 9), (9, 13), (13, 17))
FOLLOW = ((0, 4), (4, 8), (8, 12), (12, 17))
SETTLE = ((0, 3), (3, 7), (7, 11), (11, 16))
ZLO, XS, CORES, YS = 4, 4, 2, 4
PLANE, LINE = XS * YS, ZLO * 2
SUMS = 28 * 64
PART = SUMS // CORES
PIECE = PART // PLANE


def widen(wide, weight):
    def step(k):
        kt, kr = k // 3, k % 3
        none = jnp.zeros((64, 64), BF16)
        taps = [none] + [weight[3 * k + kq] for kq in range(3)] + [none]
        columns = pl.ds(pl.multiple_of(128 * kr, 128), 128)
        for a in range(4):
            block = jnp.concatenate([taps[a + 1], taps[a]], axis=1)
            wide[pl.ds(pl.multiple_of(256 * kt + 64 * a, 64), 64), columns] = block

    loop(0, 9, step)


def widen_back(wide, weight):
    def step(k):
        kt, kr = k // 3, k % 3
        none = jnp.zeros((64, 64), BF16)
        taps = [none] + [weight[3 * (8 - k) + 2 - kq] for kq in range(3)] + [none]
        for b in range(2):
            rows = pl.ds(pl.multiple_of(128 * kr + 64 * b, 64), 64)
            for a in range(0, 4, 2):
                block = jnp.concatenate([taps[a + 1 - b], taps[a + 2 - b]], axis=1)
                wide[rows, pl.ds(pl.multiple_of(256 * kt + 64 * a, 128), 128)] = block

    loop(0, 9, step)


def silu_slope(value):
    logistic = jax.nn.sigmoid(value)
    return logistic * (1.0 + value * (1.0 - logistic))


def row_of(shape):
    return lax.broadcasted_iota(jnp.int32, shape, 0) % ROWS


def row_before(block):
    return jnp.where(row_of(block.shape) == 0, 0.0, pltpu.roll(block, 1, axis=0))


def row_after(block):
    return jnp.where(row_of(block.shape) == ROWS - 1, 0.0, pltpu.roll(block, block.shape[0] - 1, axis=0))


def half_shift(block, ends=True):
    none = jnp.zeros((ROWS, 128), F32)
    turn = pltpu.roll(block, 64, axis=1)
    left, right = (jnp.concatenate([none, turn], 0), jnp.concatenate([turn, none], 0)) if ends else (turn[:-ROWS], turn[ROWS:])
    lane = lax.broadcasted_iota(jnp.int32, left.shape, 1)
    return jnp.where(lane < 64, left, right).astype(BF16)


def piece_shift(load, low, high):
    none = jnp.zeros((ROWS, 128), F32)
    blocks = [load(l).astype(F32) if 0 <= l < PAIRS else none for l in range(low - 1, high + (high == PAIRS))]
    return half_shift(jnp.concatenate(blocks, 0), False)


def flat(ref, slot):
    return jnp.concatenate([ref[slot, :, 128 * l : 128 * l + 128] for l in range(PAIRS)], axis=0).astype(F32)


def conv(ref, slots, weight, back=True, low=0, high=PAIRS):
    frames = []
    for slot in slots:
        parts = []
        for j in range(3):
            parts += [ref[slot + j, ROWS * low : ROWS * high, :], ref[slot + j, ROWS * low + ROWS : ROWS * high + ROWS, :]]
        frames.append(jnp.concatenate(parts, axis=1))
    over = (((1,), (1 if back else 0,)), ((), ()))
    sums = lax.dot_general(jnp.concatenate(frames, axis=0), weight[...], over, preferred_element_type=F32)
    return sums[:, 128:256] + row_before(sums[:, 0:128]) + row_after(sums[:, 256:384])


def three_rows(ref, slot, block):
    ref[slot, 0] = row_after(block).astype(BF16)
    ref[slot, 1] = block.astype(BF16)
    ref[slot, 2] = row_before(block).astype(BF16)


def loop(low, high, step):
    def body(i, carry):
        step(i)
        return carry

    lax.fori_loop(low, high, body, 0)


def kernel(
    factor,
    x_hbm, icache_hbm, mcache_hbm, ct_hbm, weight1_hbm, weight2_hbm, bias_hbm,
    out, icg, mcg, sums,
    weight1, weight2, bias, x, ct, mc, acts, cts, mid3, slope, mid_grad, pg, pg3, pgs, eg, dealt, passed, raw1, raw2,
    w1, w2t, w1t, vsum, from_core, plane_out, plane_in, line, whole,
    core_sem, plane_send, plane_recv, line_send, line_recv, spread_send, spread_recv, leave_sem, weight_sem,
    local_sem, send_sem, recv_sem, deal_sem, pass_send, pass_recv, own_sem,
):
    tm = lax.axis_index("tm")
    four, side = tm // 2, tm % 2
    first, last = four == 0, four == 3
    other = tm + 1 - 2 * side
    clip = lax.axis_index("clip")
    zlo, across, core = clip // (XS * CORES), (clip // CORES) % XS, clip % CORES
    spot, depth = across * YS + four, side * ZLO + zlo

    hops = lambda d, size: min(d, size - d)
    plane_steps = [(i, j) for i in range(XS) for j in range(YS) if i or j]
    plane_steps.sort(key=lambda step: -hops(step[0], XS) - hops(step[1], YS))
    line_steps = sorted(range(1, LINE), key=lambda step: -hops(step, LINE))

    def in_plane(i):
        to_x, to_y = (across + plane_steps[i - 1][0]) % XS, (four + plane_steps[i - 1][1]) % YS
        return to_x * YS + to_y, {"clip": (zlo * XS + to_x) * CORES + core, "tm": to_y * 2 + side}

    def in_line(i):
        to = (depth + line_steps[i - 1]) % LINE
        return {"clip": (to % ZLO * XS + across) * CORES + core, "tm": four * 2 + to // ZLO}

    def anyone(src, dst, send, recv, to):
        return pltpu.make_async_remote_copy(src, dst, send, recv, device_id=to, device_id_type=MESH)

    twin = {"clip": clip + 1 - 2 * core, "tm": tm}
    mine = pl.ds(pl.multiple_of(side * (15 * 128), 128), SPAN)
    theirs = pl.ds(pl.multiple_of((1 - side) * (15 * 128), 128), SPAN)
    keep = pl.ds(pl.multiple_of(side * 128, 128), HALF)
    home = pl.ds(pl.multiple_of(side * HALF, 128), HALF)

    def remote(src, dst, i, to):
        return pltpu.make_async_remote_copy(
            src, dst, send_sem.at[i], recv_sem.at[i], device_id={"tm": to}, device_id_type=MESH
        )

    here = []
    for f in range(2):
        here.append(pltpu.make_async_copy(x_hbm.at[f, :, mine], x.at[2 + 2 * side + f], local_sem.at[f]))
        here.append(pltpu.make_async_copy(ct_hbm.at[f, :, mine], ct.at[2 * side + f], local_sem.at[2 + f]))
    for copy in here:
        copy.start()
    cached = []
    for f in range(2):
        cached.append(pltpu.make_async_copy(icache_hbm.at[f, :, mine], x.at[f], local_sem.at[4 + f]))
        cached.append(pltpu.make_async_copy(mcache_hbm.at[f, :, mine], mc.at[f], local_sem.at[6 + f]))

    @pl.when(first)
    def _():
        for copy in cached:
            copy.start()

    barrier = pltpu.get_barrier_semaphore()
    for d in range(1, 8):
        pl.semaphore_signal(barrier, inc=1, device_id={"tm": (tm + d) % 8}, device_id_type=MESH)
    greeted = 8
    pl.semaphore_signal(barrier, inc=1, device_id=twin, device_id_type=MESH)
    for i in range(1, XS):
        for j in range(YS):
            to = {"clip": (zlo * XS + (across + i) % XS) * CORES + core, "tm": (four + j) % YS * 2 + side}
            pl.semaphore_signal(barrier, inc=1, device_id=to, device_id_type=MESH)
            greeted += 1
    for i in range(1, ZLO):
        for j in range(2):
            to = {"clip": ((zlo + i) % ZLO * XS + across) * CORES + core, "tm": four * 2 + (side + j) % 2}
            pl.semaphore_signal(barrier, inc=1, device_id=to, device_id_type=MESH)
            greeted += 1
    pl.semaphore_wait(barrier, greeted)

    x_swap, ct_swap, x_halo, ct_halo, pg_halo = [], [], [], [], []
    for c, ((low, high), (a, b)) in enumerate(zip(ARRIVE, FOLLOW)):
        cut = pl.ds(pl.multiple_of((1 - side) * (15 * 128) + 128 * low, 128), 128 * (high - low))
        cols = pl.ds(128 * low, 128 * (high - low))
        rows = pl.ds(ROWS * a, ROWS * (b - a))
        ours, two, four_on = pl.ds(2 * side, 2), pl.ds(0, 2), pl.ds(4, 2)
        x_swap.append(remote(x_hbm.at[:, :, cut], x.at[pl.ds(2 + 2 * side, 2), :, cols], c, other))
        ct_swap.append(remote(ct_hbm.at[:, :, cut], ct.at[ours, :, cols], 4 + c, other))
        x_halo.append(remote(x.at[four_on, :, cols], x.at[two, :, cols], 8 + c, (tm + 2) % 8))
        ct_halo.append(remote(ct.at[two, :, cols], ct.at[four_on, :, cols], 12 + c, (tm + 6) % 8))
        pg_halo.append(remote(pg.at[two, rows, :], pg.at[four_on, rows, :], 16 + c, (tm + 6) % 8))

    @pl.when(side == 0)
    def _():
        for copy in ct_swap + x_swap:
            copy.start()

    @pl.when(side == 1)
    def _():
        for copy in x_swap + ct_swap:
            copy.start()

    for copy in here:
        copy.wait()

    @pl.when((side == 1) & jnp.logical_not(last))
    def _():
        for copy in x_halo:
            copy.start()

    @pl.when((side == 0) & jnp.logical_not(first))
    def _():
        for copy in ct_halo:
            copy.start()

    weights = [
        pltpu.make_async_copy(src, dst, weight_sem.at[i])
        for i, (src, dst) in enumerate(((weight1_hbm, weight1), (weight2_hbm, weight2), (bias_hbm, bias)))
    ]
    for copy in weights:
        copy.start()
    for copy in weights:
        copy.wait()
    widen(w1, weight1)
    widen_back(w2t, weight2)
    widen_back(w1t, weight1)
    two_biases = jnp.concatenate([bias[...], bias[...]], axis=1)
    vsum[64 * TAPS :, :] = jnp.zeros((64, 128), F32)

    @pl.when(last)
    def _():
        for s in range(4, 6):
            ct[s] = jnp.zeros((ROWS, SPAN), BF16)
            pg[s] = jnp.zeros((FLAT, 128), BF16)

    for s in range(2):
        cts[s] = jnp.zeros((FLAT + ROWS, 128), BF16)
        pgs[s] = jnp.zeros((FLAT + ROWS, 128), BF16)
    raw2[...] = jnp.zeros_like(raw2)

    def forward(c):
        @pl.when(jnp.logical_not(first))
        def _():
            x_halo[c].wait_recv()

        (low, high), (a, b) = ARRIVE[c], FOLLOW[c]
        for s in range(6):
            acts[s, ROWS * low : ROWS * (high + (high == PAIRS)), :] = piece_shift(
                lambda l, s=s: jax.nn.silu(x[s, :, 128 * l : 128 * l + 128].astype(F32)), low, high
            )
        pre = conv(acts, range(4), w1, False, a, b) + two_biases
        slopes = silu_slope(pre)
        middle = jax.nn.silu(pre).astype(BF16)
        wide = middle.astype(F32)
        before, after = row_before(wide).astype(BF16), row_after(wide).astype(BF16)
        size = ROWS * (b - a)
        for t in range(4):
            here, there = slice(size * t, size * t + size), slice(ROWS * a, ROWS * b)
            slope[t, there, :] = slopes[here]
            mid3[t + 2, 0, there, :] = after[here]
            mid3[t + 2, 1, there, :] = middle[here]
            mid3[t + 2, 2, there, :] = before[here]

    over_rows = (((0,), (0,)), ((), ()))

    def operands(still, moved, frames, ahead, rows):
        one, four_px = [], []
        for n in frames:
            one.append(jnp.concatenate([still[n, v, rows[0], :] for v in range(3)], axis=1))
            four_px.append(jnp.concatenate([moved[n + ahead + j, r, :] for j in range(3) for r in rows], axis=1))
        return jnp.concatenate(one, axis=0), jnp.concatenate(four_px, axis=0)

    def own_rows(c):
        i, k = SETTLE[c]
        return [pl.ds(pl.multiple_of((side + e + i) * ROWS, ROWS), ROWS * (k - i)) for e in range(2)]

    def backward(c):
        @pl.when(jnp.logical_not(last))
        def _():
            ct_halo[c].wait_recv()

        (low, high), (a, b) = ARRIVE[c], FOLLOW[c]
        for s in range(6):
            cts[s + 2, ROWS * low : ROWS * (high + (high == PAIRS)), :] = piece_shift(
                lambda l, s=s: ct[s, :, 128 * l : 128 * l + 128], low, high
            )
        grad = conv(cts, range(2, 6), w2t, low=a, high=b)
        size = ROWS * (b - a)
        for t in range(4):
            mid_grad[t, ROWS * a : ROWS * b, :] = grad[size * t : size * t + size]

        @pl.when(first)
        def _():
            one, four_px = operands(mid3, cts, range(2), 0, own_rows(c))
            raw2[...] += lax.dot_general(one, four_px, over_rows, preferred_element_type=F32)

    def settle(c):
        a, b = FOLLOW[c]
        size = ROWS * (b - a)
        grad = jnp.concatenate([mid_grad[t, ROWS * a : ROWS * b, :] for t in range(4)], axis=0)
        grad = (grad * jnp.concatenate([slope[t, ROWS * a : ROWS * b, :] for t in range(4)], axis=0)).astype(BF16)
        wide = grad.astype(F32)
        before, after = row_before(wide).astype(BF16), row_after(wide).astype(BF16)
        for t in range(4):
            here, there = slice(size * t, size * t + size), slice(ROWS * a, ROWS * b)
            pg[t, there, :] = grad[here]
            pg3[t, 0, there, :] = after[here]
            pg3[t, 1, there, :] = grad[here]
            pg3[t, 2, there, :] = before[here]
            pgs[t + 2, ROWS * a : ROWS * (b + (b == PAIRS)), :] = piece_shift(
                lambda l, t=t: pg[t, ROWS * l : ROWS * l + ROWS, :], a, b
            )
        rows = own_rows(c)
        raw2[...] += lax.dot_general(*operands(mid3, cts, range(2, 6), 0, rows), over_rows, preferred_element_type=F32)
        one, four_px = operands(pg3, acts, range(4), 0, rows)
        sums = lax.dot_general(four_px, one, over_rows, preferred_element_type=F32)
        raw1[...] = sums if c == 0 else raw1[...] + sums

        @pl.when(jnp.logical_not(first))
        def _():
            pg_halo[c].start()

    @pl.when(first)
    def _():
        for copy in cached:
            copy.wait()
        loop(0, 2, lambda s: three_rows(mid3, s, flat(mc, s)))

    @pl.when(side == 0)
    def _():
        for c in range(5):
            if c < 4:
                x_swap[c].wait_recv()

                @pl.when(jnp.logical_not(last))
                def _():
                    x_halo[c].start()

            if c > 0:
                forward(c - 1)

    @pl.when(side == 1)
    def _():
        for c in range(5):
            if c < 4:
                ct_swap[c].wait_recv()

                @pl.when(jnp.logical_not(first))
                def _():
                    ct_halo[c].start()

            if c > 0:
                backward(c - 1)

    for c in range(4):
        @pl.when(side == 0)
        def _():
            ct_swap[c].wait_recv()
            backward(c)

        @pl.when(side == 1)
        def _():
            x_swap[c].wait_recv()
            forward(c)

        settle(c)

    def pieces(k, f, block):
        wide = jnp.concatenate([block[ROWS * l : ROWS * l + ROWS, :] for l in range(PAIRS)], axis=1)
        for p in range(8):
            dealt[p, k, f] = wide[4 * p : 4 * p + 4, :].astype(BF16)

    deals = []
    for v in range(1, YS):
        pair = dealt.at[pl.ds(2 * v, 2), :, :, :, keep]
        deals.append(anyone(pair, passed, deal_sem.at[v], deal_sem.at[0], {"tm": 2 * v + side}))

    def pass_on(held, act):
        for k, result in enumerate((mcg, icg)):
            to = result.at[:, :, home]
            near = pltpu.make_async_copy(held(side, k), to, own_sem.at[k])
            act(near, anyone(held(1 - side, k), to, pass_send.at[k], pass_recv.at[k], {"tm": other}))

    def pass_all(act):
        @pl.when(first)
        def _():
            pass_on(lambda q, k: dealt.at[q, k, :, :, keep], act)

        @pl.when(jnp.logical_not(first))
        def _():
            pass_on(lambda q, k: passed.at[q, k], act)

    def extended_gradient(n):
        return conv(pgs, [n], w1t) * silu_slope(flat(x, n))

    def input_gradient(t):
        block = extended_gradient(t + 2) + flat(ct, t)
        for l in range(PAIRS):
            eg[t, :, 128 * l : 128 * l + 128] = block[ROWS * l : ROWS * l + ROWS, :].astype(BF16)

    far = 2 - 2 * side
    back = [remote(eg.at[far + f, :, keep], out.at[f, :, home], 20 + f, other) for f in range(2)]
    stay = [pltpu.make_async_copy(eg.at[2 - far + f, :, keep], out.at[f, :, home], local_sem.at[f]) for f in range(2)]
    lane = lax.broadcasted_iota(jnp.int32, (64, 128), 1)

    def fold(taps):
        for tap in taps:
            kt, kr, kq = tap // 9, tap // 3 % 3, tap % 3
            at, one, two = 256 * kt + 64 * kq, 128 * kr, 128 * (2 - kr)
            left = raw1[at : at + 64, one : one + 128]
            left += pltpu.roll(raw1[at + 64 : at + 128, one : one + 128], 64, axis=1)
            at = 256 * (2 - kt)
            low, high = raw2[two : two + 64, at : at + 256], raw2[two + 64 : two + 128, at : at + 256]
            if kq == 1:
                right = low[:, 0:128] + pltpu.roll(high[:, 128:256], 64, axis=1)
            else:
                tile = 1 - kq // 2
                right = pltpu.roll(low[:, 128 * tile : 128 * tile + 128], 64, axis=1) + high[:, 128 * tile : 128 * tile + 128]
            vsum[64 * tap : 64 * tap + 64, :] = jnp.where(lane < 64, left, right)

    half_of = lambda c: pl.ds(pl.multiple_of(c * PART, 8), PART)
    cores = anyone(vsum.at[half_of(1 - core)], from_core, core_sem.at[0], core_sem.at[1], twin)
    for k in range(2):

        @pl.when(core == k)
        def _():
            fold(range(14 * (1 - k), min(TAPS, 28 - 14 * k)))
            cores.start()
            fold(range(14 * k, min(TAPS, 14 + 14 * k)))


    def shift_pg(s):
        pgs[s + 2] = half_shift(pg[s].astype(F32))

    def late_frames(send):
        @pl.when(jnp.logical_not(last))
        def _():
            for copy in pg_halo:
                copy.wait_recv()

        loop(4, 6, shift_pg)
        for t in range(2, 4):
            loop(t, t + 1, input_gradient)
            if send:
                back[t - 2].start()

    @pl.when(side == 1)
    def _():
        loop(0, 2, input_gradient)
        for copy in back:
            copy.start()

    cores.wait_recv()

    def part(to):
        own = pl.ds(pl.multiple_of(core * PART + to * PIECE, 8), PIECE)
        return vsum[own, :] + from_core[pl.ds(pl.multiple_of(to * PIECE, 8), PIECE), :]

    gathers = []
    for i in range(1, PLANE):
        to, device = in_plane(i)
        plane_out[i] = part(to).astype(BF16)
        gathers.append(anyone(plane_out.at[i], plane_in.at[i], plane_send.at[i], plane_recv.at[i], device))
        gathers[-1].start()
    @pl.when(side == 0)
    def _():
        late_frames(True)

    @pl.when(first)
    def _():
        loop(0, 2, lambda n: pieces(0, n, conv(cts, [n], w2t)))
        loop(0, 2, lambda n: pieces(1, n, extended_gradient(n)))
        for copy in deals:
            copy.start()

    total = part(spot)
    for i, copy in enumerate(gathers):
        copy.wait_recv()
        total += plane_in[i + 1].astype(F32)
    line[depth] = total.astype(BF16)
    lines = [anyone(line.at[depth], line.at[depth], line_send.at[i], line_recv.at[i], in_line(i)) for i in range(1, LINE)]
    for copy in lines:
        copy.start()
    @pl.when(side == 0)
    def _():
        loop(0, 2, input_gradient)

    @pl.when(side == 1)
    def _():
        late_frames(False)

    for copy in stay:
        copy.start()
    for copy in lines:
        copy.wait_recv()
    total = line[0].astype(F32)
    for i in range(1, LINE):
        total += line[i].astype(F32)
    whole[core, spot] = (total * factor).astype(BF16)
    spreads = []
    for i in range(1, PLANE):
        to, device = in_plane(i)
        spreads.append(anyone(whole.at[core, spot], whole.at[core, spot], spread_send.at[i], spread_recv.at[i], device))
    for copy in spreads:
        copy.start()

    @pl.when(jnp.logical_not(first))
    def _():
        deals[0].wait_recv()

    pass_all(lambda near, far: (near.start(), far.start()))
    for copy in spreads:
        copy.wait_recv()
    twins = anyone(whole.at[core], whole.at[core], core_sem.at[2], core_sem.at[3], twin)
    twins.start()
    leave = [pltpu.make_async_copy(whole.at[h], sums.at[h], leave_sem.at[e]) for e, h in enumerate((core, 1 - core))]
    leave[0].start()
    twins.wait_recv()
    leave[1].start()
    for copy in stay:
        copy.wait()
    for copy in x_swap + ct_swap + [cores, twins] + gathers + lines + spreads:
        copy.wait_send()

    @pl.when(jnp.logical_not(last))
    def _():
        for copy in x_halo:
            copy.wait_send()

    @pl.when(jnp.logical_not(first))
    def _():
        for copy in ct_halo + pg_halo:
            copy.wait_send()

    back[0].wait_recv()
    back[1].wait_recv()
    for copy in back:
        copy.wait_send()
    @pl.when(first)
    def _():
        for copy in deals:
            copy.wait_send()

    for copy in leave:
        copy.wait()
    pass_all(lambda near, far: (near.wait(), far.wait()))


def deliver(
    out_in, icg_in, mcg_in, sums_in, out, icg, mcg, grad1, grad2, out_at, icg_at, mcg_at, sums_at, one, two, in_sem, out_sem
):
    loads = [
        pltpu.make_async_copy(src, dst, in_sem.at[i])
        for i, (src, dst) in enumerate(((sums_in, sums_at), (out_in, out_at), (icg_in, icg_at), (mcg_in, mcg_at)))
    ]
    stores = [
        pltpu.make_async_copy(src, dst, out_sem.at[i])
        for i, (src, dst) in enumerate(((out_at, out), (icg_at, icg), (mcg_at, mcg)))
    ]
    for copy in loads:
        copy.start()
    loads[0].wait()
    for k in range(3):
        part = pl.ds(9 * k, 9)
        block = sums_at[...].astype(F32).reshape(SUMS, 128)[576 * k : 576 * k + 576]
        turned_block = pltpu.roll(block, 64, axis=1)
        for tap in range(9):
            one[9 * k + tap] = block[64 * tap : 64 * tap + 64, 0:64]
            two[9 * k + tap] = turned_block[64 * tap : 64 * tap + 64, 0:64]
        stores.append(pltpu.make_async_copy(one.at[part], grad1.at[part], out_sem.at[3 + 2 * k]))
        stores.append(pltpu.make_async_copy(two.at[part], grad2.at[part], out_sem.at[4 + 2 * k]))
        for copy in stores[-2:]:
            copy.start()
    for load, store in zip(loads[1:], stores[:3]):
        load.wait()
        store.start()
    for copy in stores:
        copy.wait()


def body(block_input, input_cache, middle_cache, first_weight, first_bias, second_weight, cotangent):
    count = 1024 * lax.axis_size("clip") * lax.axis_size("tm") * 4
    anywhere = pl.BlockSpec(memory_space=pl.ANY)
    results = pl.pallas_call(
        functools.partial(kernel, 1.0 / math.sqrt(count)),
        out_shape=(
            jax.ShapeDtypeStruct((2, ROWS, 4096), BF16),
            jax.ShapeDtypeStruct((2, 4, 4096), BF16),
            jax.ShapeDtypeStruct((2, 4, 4096), BF16),
            jax.ShapeDtypeStruct((CORES, PLANE, PIECE, 128), BF16),
        ),
        in_specs=[anywhere] * 7,
        out_specs=(anywhere,) * 4,
        scratch_shapes=[
            pltpu.VMEM((TAPS, 64, 64), BF16),
            pltpu.VMEM((TAPS, 64, 64), BF16),
            pltpu.VMEM((1, 64), F32),
            pltpu.VMEM((6, ROWS, SPAN), BF16),
            pltpu.VMEM((6, ROWS, SPAN), BF16),
            pltpu.VMEM((2, ROWS, SPAN), BF16),
            pltpu.VMEM((6, FLAT + ROWS, 128), BF16),
            pltpu.VMEM((8, FLAT + ROWS, 128), BF16),
            pltpu.VMEM((6, 3, FLAT, 128), BF16),
            pltpu.VMEM((4, FLAT, 128), F32),
            pltpu.VMEM((4, FLAT, 128), F32),
            pltpu.VMEM((6, FLAT, 128), BF16),
            pltpu.VMEM((4, 3, FLAT, 128), BF16),
            pltpu.VMEM((8, FLAT + ROWS, 128), BF16),
            pltpu.VMEM((4, ROWS, SPAN), BF16),
            pltpu.VMEM((8, 2, 2, 4, SPAN), BF16),
            pltpu.VMEM((2, 2, 2, 4, HALF), BF16),
            pltpu.VMEM((768, 384), F32),
            pltpu.VMEM((384, 768), F32),
            pltpu.VMEM((768, 384), BF16),
            pltpu.VMEM((384, 768), BF16),
            pltpu.VMEM((384, 768), BF16),
            pltpu.VMEM((SUMS, 128), F32),
            pltpu.VMEM((PART, 128), F32),
            pltpu.VMEM((PLANE, PIECE, 128), BF16),
            pltpu.VMEM((PLANE, PIECE, 128), BF16),
            pltpu.VMEM((LINE, PIECE, 128), BF16),
            pltpu.VMEM((CORES, PLANE, PIECE, 128), BF16),
            pltpu.SemaphoreType.DMA((4,)),
            pltpu.SemaphoreType.DMA((PLANE,)),
            pltpu.SemaphoreType.DMA((PLANE,)),
            pltpu.SemaphoreType.DMA((LINE,)),
            pltpu.SemaphoreType.DMA((LINE,)),
            pltpu.SemaphoreType.DMA((PLANE,)),
            pltpu.SemaphoreType.DMA((PLANE,)),
            pltpu.SemaphoreType.DMA((2,)),
            pltpu.SemaphoreType.DMA((3,)),
            pltpu.SemaphoreType.DMA((8,)),
            pltpu.SemaphoreType.DMA((22,)),
            pltpu.SemaphoreType.DMA((22,)),
            pltpu.SemaphoreType.DMA((YS,)),
            pltpu.SemaphoreType.DMA((2,)),
            pltpu.SemaphoreType.DMA((2,)),
            pltpu.SemaphoreType.DMA((2,)),
        ],
        compiler_params=pltpu.CompilerParams(
            collective_id=0, has_side_effects=True, vmem_limit_bytes=56 << 20
        ),
    )(
        block_input[0], input_cache[0], middle_cache[0], cotangent[0],
        first_weight.reshape(TAPS, 64, 64), second_weight.reshape(TAPS, 64, 64), first_bias.reshape(1, 64),
    )
    out, icg, mcg, grad1, grad2 = pl.pallas_call(
        deliver,
        out_shape=(
            jax.ShapeDtypeStruct((2, ROWS, 4096), BF16),
            jax.ShapeDtypeStruct((2, 4, 4096), BF16),
            jax.ShapeDtypeStruct((2, 4, 4096), BF16),
            jax.ShapeDtypeStruct((TAPS, 64, 64), F32),
            jax.ShapeDtypeStruct((TAPS, 64, 64), F32),
        ),
        in_specs=[anywhere] * 4,
        out_specs=(anywhere,) * 5,
        scratch_shapes=[
            pltpu.VMEM((2, ROWS, 4096), BF16),
            pltpu.VMEM((2, 4, 4096), BF16),
            pltpu.VMEM((2, 4, 4096), BF16),
            pltpu.VMEM((CORES, PLANE, PIECE, 128), BF16),
            pltpu.VMEM((TAPS, 64, 64), F32),
            pltpu.VMEM((TAPS, 64, 64), F32),
            pltpu.SemaphoreType.DMA((4,)),
            pltpu.SemaphoreType.DMA((9,)),
        ],
    )(*results)
    shape = (3, 3, 3, 64, 64)
    return (out[None], icg[None], mcg[None], grad1.reshape(shape), grad2.reshape(shape))


def solution(mesh):
    return jax.shard_map(
        body,
        mesh=mesh,
        in_specs=(
            P("clip", "tm", None, None),
            P("clip", None, None, None),
            P("clip", None, None, None),
            P(),
            P(),
            P(),
            P("clip", "tm", None, None),
        ),
        out_specs=(
            P("clip", "tm", None, None),
            P("clip", None, "tm", None),
            P("clip", None, "tm", None),
            P(),
            P(),
        ),
        check_vma=False,
    )
```
